128 devices in a mesh: row: 8 (over x_lo, z), col: 16 (over x_hi, y, core).
Axes of the slice: x: 4 (x_hi: 2, x_lo: 2; x = x_hi * 2 + x_lo), y: 4, z: 4, core: 2. Of those that a mesh axis runs over, the one named last changes fastest.
Arguments:
- loadings: float32 [64, 32, 16384], P(None, None, ('row', 'col')), may hold values from -6 to 6
Outputs:
- correlation: float32 [16384, 16384], P('row', 'col')
The draws below stay inside these ranges and needn't reach their ends.
All inputs are finite; a program needn't handle non-finite values.
Results may differ from the reference program's by a relative error of at most 0.000096.
Values sent between devices are 32-bit elements; how exact they have to be, the bound alone decides.
No kernel may reach another device: no remote copies, remote signals or barrier semaphores. Data moves between devices by JAX's collectives and lax.ppermute only.
A program may use at most 128 MiB of HBM per device.

```python
import jax
import jax.numpy as jnp
from jax import lax

SPECIES = 16384
FACTORS = 32
SAMPLES = 64


def shard_levels(own_key, extent, split, low, top_value):
    def one(axis_at, blocks):
        draws = jax.random.uniform(jax.random.fold_in(jax.random.fold_in(own_key, 6), axis_at), (blocks,), jnp.float32, low / len(split), top_value / len(split))
        return jnp.repeat(jnp.exp(draws), extent[axis_at] // blocks).reshape((-1,) + (1,) * (len(extent) - axis_at - 1))

    factor_of = one(*split[0])
    for cut in split[1:]:
        factor_of = factor_of * one(*cut)
    return factor_of


def gaussian(key, dims, width, most, pieces=(), held_as=jnp.bfloat16):
    factor_of = shard_levels(key, dims, pieces, -0.22, 0.18) if pieces else 1.0
    array = jax.random.normal(key, dims, jnp.float32) * width * factor_of
    return jnp.minimum(jnp.maximum(array, -most), most).astype(held_as)


def setup_inputs(seed: int = 0) -> dict:
    streams_of = jax.random.split(jax.random.key(seed), 2)
    return {
        "loadings": gaussian(streams_of[0], (SAMPLES, FACTORS, SPECIES), 1.0, 6.0, ((2, 128),), jnp.float32),
    }


def reference(loadings):
    variance = lax.optimization_barrier(jnp.sum(loadings * loadings, axis=1, keepdims=True))
    scaled = loadings / jnp.sqrt(variance)
    flat = scaled.reshape(SAMPLES * FACTORS, SPECIES)
    total = jnp.dot(flat.T, flat, precision=lax.Precision.HIGHEST, preferred_element_type=jnp.float32)
    return total * (1.0 / SAMPLES)
```

```python
import jax
import jax.numpy as jnp
from jax import lax
from jax.sharding import PartitionSpec as P


def column_pairs(rows, cols):
    halves = cols // rows
    pairs = []
    for r in range(rows):
        for c in range(cols):
            pairs.append(((c // halves) * cols + (c % halves) * rows + r, r * cols + c))
    return pairs


def local(loadings):
    count, factors, width = loadings.shape
    depth = count * factors
    variance = jnp.sum(loadings * loadings, axis=1, keepdims=True)
    scaled = loadings / jnp.sqrt(variance)
    pairs = column_pairs(lax.axis_size("row"), lax.axis_size("col"))
    moved = lax.ppermute(scaled, ("row", "col"), pairs)
    right = lax.all_gather(moved, "row", axis=2, tiled=True)
    left = lax.all_gather(scaled, "col", axis=2, tiled=True)
    total = lax.dot_general(
        left.reshape(depth, -1),
        right.reshape(depth, -1),
        (((0,), (0,)), ((), ())),
        precision=lax.Precision.HIGH,
        preferred_element_type=jnp.float32,
    )
    return total * (1.0 / count)


def solution(mesh):
    placed = (P(None, None, ("row", "col")),)
    return jax.shard_map(
        local, mesh=mesh, in_specs=placed, out_specs=P("row", "col"), check_vma=False
    )
```
